16 devices in a mesh: rep: 1, r: 4 (over y, z), s: 4 (over x, core).
Axes of the slice: x: 2, y: 2, z: 2, core: 2. Of those that a mesh axis runs over, the one named last changes fastest.
Arguments:
- x: bfloat16 [16, 4096, 640], P(('rep', 'r', 's'))
- dy: bfloat16 [16, 4096, 640], P(('rep', 'r', 's'))
- w_gate: bfloat16 [2, 640, 3200], P(None, 's')
- w_up: bfloat16 [2, 640, 3200], P(None, 's')
- w_down: bfloat16 [2, 3200, 640], P(None, 's')
- m_w_gate: float32 [2, 640, 3200], P(None, 's')
- m_w_up: float32 [2, 640, 3200], P(None, 's')
- m_w_down: float32 [2, 3200, 640], P(None, 's')
- v_w_gate: float32 [2, 640, 3200], P(None, 's')
- v_w_up: float32 [2, 640, 3200], P(None, 's')
- v_w_down: float32 [2, 3200, 640], P(None, 's')
Outputs:
- output 1: bfloat16 [2, 640, 3200], P('rep', 's')
- output 2: bfloat16 [2, 640, 3200], P('rep', 's')
- output 3: bfloat16 [2, 3200, 640], P('rep', 's')
- output 4: float32 [2, 640, 3200], P('rep', 's')
- output 5: float32 [2, 640, 3200], P('rep', 's')
- output 6: float32 [2, 3200, 640], P('rep', 's')
- output 7: float32 [2, 640, 3200], P('rep', 's')
- output 8: float32 [2, 640, 3200], P('rep', 's')
- output 9: float32 [2, 3200, 640], P('rep', 's')
All inputs are finite; a program needn't handle non-finite values.
Results may differ from the reference program's by a relative error of at most 0.022.
Values are sent between devices in bfloat16 or wider.
A program may use at most 2 GiB of HBM per device.

```python
import jax
import jax.numpy as jnp
from jax import lax

SEQUENCES = 16
TOKENS = 4096
D = 640
FF = 3200
LAYERS = 2
NAMES = ("w_gate", "w_up", "w_down")
SHAPES = {"w_gate": (LAYERS, D, FF), "w_up": (LAYERS, D, FF), "w_down": (LAYERS, FF, D)}


def bump(key, n, height):
    away = (jnp.arange(n, dtype=jnp.int32) - jax.random.randint(key, (), 0, n, jnp.int32)) % n
    return jnp.where(away < n // 8, height, 1.0)


def together(key, own, strength):
    shared = jax.random.normal(key, own.shape[1:], jnp.float32)
    return (own + strength * shared) * lax.rsqrt(1 + strength * strength)


def setup_inputs(seed: int = 0, part: int = 0) -> dict:
    kx, kdy, ka, kb, kz, kf, kh, kl, *keys = jax.random.split(jax.random.key(seed), 8 + 3 * len(NAMES))
    kx, kdy, ka, kb = (jax.random.fold_in(k, part) for k in (kx, kdy, ka, kb))
    kw, km, kv = (keys[i::3] for i in range(3))
    shape = (SEQUENCES, TOKENS, D)
    much_x, much_dy = jax.random.uniform(kz, (2,), jnp.float32, 0.0, 1.0)
    loud = 2.0 ** jax.random.uniform(jax.random.fold_in(kz, 1), (), jnp.float32, -1.0, 2.0)
    layers = 2.0 ** jax.random.uniform(kl, (LAYERS, 1, 1), jnp.float32, -1.0, 1.0)
    x = together(ka, jax.random.normal(kx, shape, jnp.float32), much_x) * bump(kf, D, 4.0)
    dy = together(kb, jax.random.normal(kdy, shape, jnp.float32), much_dy)
    drawn = {"x": x.astype(jnp.bfloat16), "dy": (loud * dy * (SEQUENCES * TOKENS) ** -0.5).astype(jnp.bfloat16)}
    for key, name in zip(kw, NAMES, strict=True):
        w = jax.random.normal(key, SHAPES[name], jnp.float32) * SHAPES[name][1] ** -0.5
        drawn[name] = (w * {"w_gate": 1.0, "w_up": bump(kh, FF, 4.0), "w_down": layers}[name]).astype(jnp.bfloat16)
    for key, name in zip(km, NAMES, strict=True):
        drawn[f"m_{name}"] = 0.1 * jax.random.normal(key, SHAPES[name], jnp.float32)
    for key, name in zip(kv, NAMES, strict=True):
        drawn[f"v_{name}"] = jax.random.uniform(key, SHAPES[name], jnp.float32, 0.005, 0.015)
    return drawn


def matmul(a, w):
    return jnp.dot(a, w, preferred_element_type=jnp.float32).astype(jnp.bfloat16)


def normed(h):
    wide = h.astype(jnp.float32)
    scale = lax.rsqrt(jnp.mean(wide**2, -1, keepdims=True) + 1e-6)
    return (wide * scale).astype(jnp.bfloat16)


def layer(h, w):
    a = normed(h)
    gate = jnp.dot(a, w["w_gate"], preferred_element_type=jnp.float32)
    up = jnp.dot(a, w["w_up"], preferred_element_type=jnp.float32)
    return h + matmul((jax.nn.silu(gate) * up).astype(jnp.bfloat16), w["w_down"])


def adamw(w, m, v, g):
    m = 0.9 * m + 0.1 * g
    v = 0.95 * v + 0.05 * g * g
    step = m * lax.rsqrt(v + 1e-8) + 0.1 * w
    return (w - 0.02 * step).astype(jnp.bfloat16), m, v


def clipped(gradients, sum_of_squares, count):
    factor = jnp.minimum(1.0, 0.5 * lax.rsqrt(sum_of_squares / count + 1e-30))
    return [g * factor for g in gradients]


def stack(weights, h):
    return lax.scan(lambda h, w: (layer(h, w), None), h, weights)[0]


def reference(x, dy, w_gate, w_up, w_down, m_w_gate, m_w_up, m_w_down, v_w_gate, v_w_up, v_w_down):
    weights = dict(zip(NAMES, (w_gate, w_up, w_down), strict=True))

    def take(so_far, sequence):
        h, by_y = sequence
        _, back = jax.vjp(lambda w: stack(w, h), weights)
        return jax.tree.map(lambda total, term: total + term.astype(jnp.float32), so_far, back(by_y)[0]), None

    none_yet = {name: jnp.zeros(w.shape, jnp.float32) for name, w in weights.items()}
    by_weights, _ = lax.scan(take, none_yet, (x, dy))
    gradients = [by_weights[name].astype(jnp.bfloat16).astype(jnp.float32) for name in NAMES]
    gradients = clipped(gradients, sum(jnp.sum(g * g) for g in gradients), sum(g.size for g in gradients))
    new = [
        adamw(w.astype(jnp.float32), m, v, g)
        for w, m, v, g in zip((w_gate, w_up, w_down), (m_w_gate, m_w_up, m_w_down), (v_w_gate, v_w_up, v_w_down), gradients, strict=True)
    ]
    return tuple(one[which] for which in range(3) for one in new)
```

```python
import functools

import jax
import jax.numpy as jnp
from jax import lax
from jax.experimental import pallas as pl
from jax.experimental.pallas import tpu as pltpu
from jax.sharding import PartitionSpec as P


BF, F32 = jnp.bfloat16, jnp.float32
LANES = 128
TOKENS_PER_STEP = 512
CHUNKS = (((0, 256),), ((256, 256),), ((512, 128), (640, 32)), ((672, 128),))
VMEM = pltpu.VMEM
ANY = pl.ANY


def params(**kw):
    return pltpu.CompilerParams(vmem_limit_bytes=60 * 2**20, dimension_semantics=("arbitrary",), **kw)


def units(runs):
    return sum(n for _, n in runs)


def dot(a, b):
    return jnp.dot(a, b, preferred_element_type=F32)


def dot_nt(a, b):
    return lax.dot_general(a, b, (((1,), (1,)), ((), ())), preferred_element_type=F32)


def scale_of(wide):
    return lax.rsqrt(jnp.mean(wide * wide, -1, keepdims=True) + 1e-6)


def sigmoid(x):
    return 0.5 * jnp.tanh(0.5 * x) + 0.5


def pack_kernel(gate_ref, up_ref, down_ref, *outs):
    rows = gate_ref.shape[1]
    for runs, out in zip(CHUNKS, outs):
        row = 0
        for ref in (gate_ref, up_ref):
            for first, n in runs:
                parts = [ref[0, :, pl.ds(s * 800 + first, n)] for s in range(4)]
                parts = [jnp.concatenate(parts, -1)] if n < LANES else [p[:, t : t + LANES] for p in parts for t in range(0, n, LANES)]
                for part in parts:
                    out[pl.ds(row, rows), :] = part
                    row += rows
        first, n = runs[0][0], units(runs)
        for t in range(down_ref.shape[2] // LANES):
            out[pl.ds(row, n), :] = down_ref[0, pl.ds(first, n), pl.ds(t * LANES, LANES)]
            row += n


def pack(l, gate, up, down):
    spec = lambda w: pl.BlockSpec((1, *w.shape[1:]), lambda i: (l, 0, 0))
    shapes = [jax.ShapeDtypeStruct((15 * units(runs), LANES), BF) for runs in CHUNKS]
    return pl.pallas_call(
        pack_kernel,
        name=f"pack{l}",
        grid=(1,),
        in_specs=[spec(w) for w in (gate, up, down)],
        out_specs=[pl.BlockSpec(o.shape, lambda i: (0, 0)) for o in shapes],
        out_shape=shapes,
        compiler_params=params(),
        cost_estimate=pl.CostEstimate(flops=10**9, bytes_accessed=6 * 2**20, transcendentals=0),
    )(gate, up, down)


def partners(s):
    swap = lambda i: i + 1 - 2 * lax.rem(i, 2)
    far = lax.rem(s + 2, 4)
    return s, swap(s), far, swap(far)


def fetch(slots, wgu, wd, sems, runs):
    f = units(runs)
    tiles = 8 * f // LANES
    rows = 160
    copies = []
    for s, slot in zip(partners(lax.axis_index("s")), slots):
        if wgu is not None:
            at = pl.ds(pl.multiple_of(s * rows, 32), rows)
            for t in range(tiles):
                copies.append(pltpu.make_async_copy(slot.at[pl.ds(t * rows, rows)], wgu.at[at, pl.ds(t * LANES, LANES)], sems.at[0]))
        for t in range(5):
            row, place = tiles * rows + t * f, 0
            for _, n in runs:
                at = pl.ds(pl.multiple_of(place + s * n, 32), n)
                copies.append(pltpu.make_async_copy(slot.at[pl.ds(row, n)], wd.at[at, pl.ds(t * LANES, LANES)], sems.at[1]))
                row, place = row + n, place + 4 * n
    for copy in copies:
        copy.start()
    if wgu is not None:
        pltpu.make_async_copy(wgu, wgu, sems.at[0]).wait()
    pltpu.make_async_copy(wd, wd, sems.at[1]).wait()


def pieces(width):
    return [(c, min(512, width - c)) for c in range(0, width, 512)]


def deliver(acc_gu, acc_d, turned, keep, send, runs):
    f = units(runs)
    tiles, rows = 8 * f // LANES, 160
    turned[...] = acc_d[...].T
    for k, s in enumerate(partners(lax.axis_index("s"))):
        out = (send if k % 2 else keep).at[k // 2]
        at = pl.ds(pl.multiple_of(s * rows, 32), rows)
        for t in range(tiles):
            out[pl.ds(t * rows, rows), :] = acc_gu[at, pl.ds(t * LANES, LANES)].astype(BF)
        for t in range(5):
            row, place = tiles * rows + t * f, 0
            for _, n in runs:
                at_d = pl.ds(pl.multiple_of(place + s * n, 32), n)
                out[pl.ds(row, n), :] = turned[at_d, pl.ds(t * LANES, LANES)].astype(BF)
                row, place = row + n, place + 4 * n


def cuts(rows, shares):
    ends = [0]
    for share in shares:
        ends.append(ends[-1] + share)
    ends = [rows * e // ends[-1] // 16 * 16 for e in ends]
    return [(a, b - a) for a, b in zip(ends, ends[1:])]


class Flow:
    def __init__(self, shares, keep, send, out, squares, own, got, far, local_sem, send_sems, recv_sems):
        self.keep, self.send, self.out, self.squares, self.own, self.got, self.far = keep, send, out, squares, own, got, far
        self.local_sem, self.send_sems, self.recv_sems = local_sem, send_sems, recv_sems
        self.cuts = cuts(own.shape[1], shares)
        _, core, x, _ = partners(lax.axis_index("s"))
        _, z, y, _ = partners(lax.axis_index("r"))
        self.targets = [{"s": x}, {"r": y}, {"r": z}, {"s": core}]

    def enter(self):
        barrier = pltpu.get_barrier_semaphore()
        for target in self.targets:
            pl.semaphore_signal(barrier, inc=1, device_id=target, device_id_type=pl.DeviceIdType.MESH)
        pl.semaphore_wait(barrier, 4)
        self.local().start()
        self.near().start()

    def local(self):
        return pltpu.make_async_copy(self.keep, self.own, self.local_sem)

    def remote(self, src, dst, sem, target):
        return pltpu.make_async_remote_copy(
            src_ref=src, dst_ref=dst, send_sem=self.send_sems.at[sem], recv_sem=self.recv_sems.at[sem],
            device_id=self.targets[target], device_id_type=pl.DeviceIdType.MESH,
        )

    def near(self):
        return self.remote(self.send, self.got, 0, 3)

    def hop(self, stage, p):
        at = pl.ds(*self.cuts[p])
        return self.remote(self.own.at[0 if stage else 1, at], self.far.at[stage, at], 1 + stage * len(self.cuts) + p, stage)

    def rows(self, p):
        first, n = self.cuts[p]
        return [pl.ds(first + i, min(160, n - i)) for i in range(0, n, 160)]

    def add_near(self):
        self.local().wait()
        self.near().wait()
        for p in range(len(self.cuts)):
            for at in self.rows(p):
                self.own[1, at, :] = (self.own[1, at, :].astype(F32) + self.got[1, at, :].astype(F32)).astype(BF)

    def add_far(self, stage, p):
        self.hop(stage, p).wait()
        for at in self.rows(p):
            total = self.own[0, at, :].astype(F32) + self.far[stage, at, :].astype(F32)
            if stage == 0:
                total = total + self.got[0, at, :].astype(F32)
            total = total.astype(BF)
            if stage < 2:
                self.own[0, at, :] = total
            else:
                self.out[at, :] = total
                wide = total.astype(F32)
                self.squares[...] += jnp.sum((wide * wide).reshape(-1, 8, LANES), 0)

    def at_start(self, step):
        @pl.when(step == 0)
        def _():
            self.squares[...] = jnp.zeros_like(self.squares)
            self.enter()

        @pl.when(step == 1)
        def _():
            for p in range(len(self.cuts)):
                self.hop(0, p).start()

        for p in range(len(self.cuts)):
            for stage in (1, 2):

                @pl.when(step == 1 + p + stage)
                def _(p=p, stage=stage):
                    self.hop(stage, p).start()

    def at_end(self, step):
        @pl.when(step == 0)
        def _():
            self.add_near()

        for p in range(len(self.cuts)):
            for stage in range(3):

                @pl.when(step == 1 + p + stage)
                def _(p=p, stage=stage):
                    self.add_far(stage, p)


SHARES = (1, 1, 2, 2, 2)
TAIL_SHARES = (1,) * 6


def flow_scratch(rows, shares):
    sems = pltpu.SemaphoreType.DMA((1 + 3 * len(shares),))
    return [VMEM((2, rows, LANES), BF), VMEM((2, rows, LANES), BF), VMEM((3, rows, LANES), BF), pltpu.SemaphoreType.DMA, sems, sems]


def tail_kernel(count, parts, keep, send, *refs):
    sums, (out, factor_ref, own, got, far, local_sem, send_sems, recv_sems, squares, theirs, s_sems, r_sems) = refs[:parts], refs[parts:]
    flow = Flow(TAIL_SHARES, keep, send, out, squares, own, got, far, local_sem, send_sems, recv_sems)
    squares[...] = sums[0][...]
    for part in sums[1:]:
        squares[...] += part[...]
    flow.enter()
    flow.add_near()
    n = len(TAIL_SHARES)
    for p in range(n):
        flow.hop(0, p).start()
    for tick in range(n + 2):
        for stage in (2, 1, 0):
            p = tick - stage
            if 0 <= p < n:
                flow.add_far(stage, p)
                if stage < 2:
                    flow.hop(stage + 1, p).start()
    for i, target in enumerate((3, 0)):
        copy = pltpu.make_async_remote_copy(
            src_ref=squares.at[...] if i == 0 else theirs.at[2], dst_ref=theirs.at[i], send_sem=s_sems.at[i], recv_sem=r_sems.at[i],
            device_id=flow.targets[target], device_id_type=pl.DeviceIdType.MESH,
        )
        copy.start()
        copy.wait()
        if i == 0:
            theirs[2] = squares[...] + theirs[0]
        else:
            theirs[3] = theirs[2] + theirs[1]
    total = jnp.sum(theirs[3])
    factor_ref[...] = jnp.minimum(1.0, 0.5 * lax.rsqrt(jnp.full(factor_ref.shape, total, F32) / count + 1e-30))


def tail_call(count, keep, send, sums, ident):
    rows = keep.shape[1]
    vmem = pl.BlockSpec(memory_space=VMEM)
    return pl.pallas_call(
        functools.partial(tail_kernel, count, len(sums)),
        name="tail",
        in_specs=[pl.BlockSpec(memory_space=ANY)] * 2 + [vmem] * len(sums),
        out_specs=[vmem] * 2,
        out_shape=[jax.ShapeDtypeStruct((rows, LANES), BF), jax.ShapeDtypeStruct((8, LANES), F32)],
        scratch_shapes=flow_scratch(rows, TAIL_SHARES)
        + [VMEM((8, LANES), F32), VMEM((4, 8, LANES), F32), pltpu.SemaphoreType.DMA((2,)), pltpu.SemaphoreType.DMA((2,))],
        compiler_params=pltpu.CompilerParams(vmem_limit_bytes=60 * 2**20, collective_id=ident, has_side_effects=True),
    )(keep, send, *sums)


def forward_kernel(runs, first, last, *refs):
    refs = list(refs)
    x_ref = refs.pop(0)
    y_in = None if first else refs.pop(0)
    slots = [refs.pop(0) for _ in range(4)]
    gate_ref, up_ref = refs.pop(0), refs.pop(0)
    outs = [refs.pop(0) for _ in range(2 if last else 1)]
    wgu, wd, prod_ref, sems = refs
    width = 4 * units(runs)

    @pl.when(pl.program_id(0) == 0)
    def _():
        fetch(slots, wgu, wd, sems, runs)

    wide = x_ref[...].astype(F32)
    a = (wide * scale_of(wide)).astype(BF)
    for c, n in pieces(width):
        g = dot(a, wgu[:, pl.ds(c, n)])
        u = dot(a, wgu[:, pl.ds(width + c, n)])
        gate_ref[:, pl.ds(c, n)] = g
        up_ref[:, pl.ds(c, n)] = u
        prod_ref[:, pl.ds(c, n)] = (g * sigmoid(g) * u).astype(BF)
    y = dot(prod_ref[...], wd[...])
    if not first:
        y = y + y_in[...]
    if last:
        h = (wide + y.astype(BF).astype(F32)).astype(BF)
        outs[0][...] = h
        wide = h.astype(F32)
        outs[1][...] = (wide * scale_of(wide)).astype(BF)
    else:
        outs[0][...] = y


def swiglu_back(g, u, dp):
    dp = dp.astype(BF).astype(F32)
    sig = sigmoid(g)
    act = g * sig
    return (act * u).astype(BF), (dp * u * (sig + act * (1.0 - sig))).astype(BF), (dp * act).astype(BF)


def last_kernel(runs, first, last, *refs):
    refs = list(refs)
    a_ref, dy_ref = refs.pop(0), refs.pop(0)
    da_in = None if first else refs.pop(0)
    h_ref = refs.pop(0) if last else None
    slots = [refs.pop(0) for _ in range(4)]
    out_ref, keep, send = refs.pop(0), refs.pop(0), refs.pop(0)
    wgu, wd, acc_gu, acc_d, turned, at_ref, dyt_ref, sems, dcat = refs
    width = 4 * units(runs)

    @pl.when(pl.program_id(0) == 0)
    def _():
        acc_gu[...] = jnp.zeros_like(acc_gu)
        acc_d[...] = jnp.zeros_like(acc_d)
        fetch(slots, wgu, wd, sems, runs)

    a, dy = a_ref[...], dy_ref[...]
    at_ref[...] = a.T
    dyt_ref[...] = dy.T
    for c, n in pieces(width):
        g = dot(a, wgu[:, pl.ds(c, n)])
        u = dot(a, wgu[:, pl.ds(width + c, n)])
        dp = dot_nt(dy, wd[pl.ds(c, n), :])
        prod, dg, du = swiglu_back(g, u, dp)
        dcat[:, pl.ds(c, n)], dcat[:, pl.ds(width + c, n)] = dg, du
        acc_d[:, pl.ds(c, n)] += dot(dyt_ref[...], prod)
        acc_gu[:, pl.ds(c, n)] += dot(at_ref[...], dg)
        acc_gu[:, pl.ds(width + c, n)] += dot(at_ref[...], du)
    da = dot_nt(dcat[...], wgu[...])
    if not first:
        da = da + da_in[...]
    if last:
        da = da.astype(BF).astype(F32)
        wide = h_ref[...].astype(F32)
        scale = scale_of(wide)
        by_scale = jnp.mean(da * wide, -1, keepdims=True)
        by_h = (da * scale - wide * (scale * scale * scale * by_scale)).astype(BF)
        out_ref[...] = (dy.astype(F32) + by_h.astype(F32)).astype(BF)
    else:
        out_ref[...] = da

    @pl.when(pl.program_id(0) == pl.num_programs(0) - 1)
    def _():
        deliver(acc_gu, acc_d, turned, keep, send, runs)


def first_back_kernel(runs, *refs):
    x_ref, dh_ref, gate_ref, up_ref, *refs = refs
    slots, (keep, send, wd, acc_gu, acc_d, turned, at_ref, dht_ref, sems) = refs[:4], refs[4:]
    width = 4 * units(runs)

    @pl.when(pl.program_id(0) == 0)
    def _():
        acc_gu[...] = jnp.zeros_like(acc_gu)
        acc_d[...] = jnp.zeros_like(acc_d)
        fetch(slots, None, wd, sems, runs)

    wide = x_ref[...].astype(F32)
    a = (wide * scale_of(wide)).astype(BF)
    dh = dh_ref[...]
    at_ref[...] = a.T
    dht_ref[...] = dh.T
    for c, n in pieces(width):
        dp = dot_nt(dh, wd[pl.ds(c, n), :])
        g, u = gate_ref[:, pl.ds(c, n)], up_ref[:, pl.ds(c, n)]
        prod, dg, du = swiglu_back(g, u, dp)
        acc_d[:, pl.ds(c, n)] += dot(dht_ref[...], prod)
        acc_gu[:, pl.ds(c, n)] += dot(at_ref[...], dg)
        acc_gu[:, pl.ds(width + c, n)] += dot(at_ref[...], du)

    @pl.when(pl.program_id(0) == pl.num_programs(0) - 1)
    def _():
        deliver(acc_gu, acc_d, turned, keep, send, runs)


def call(kernel, name, tokens, blocked, slots, outs, whole, scratch, flops, aliases=None, carried=None, ident=None):
    tb = TOKENS_PER_STEP
    by_token = lambda width: pl.BlockSpec((tb, width), lambda i: (i, 0))
    shape = jax.ShapeDtypeStruct
    extra, added, more = [], [], []
    if carried:
        rows = carried[0].shape[1]
        extra, more = list(carried), flow_scratch(rows, SHARES)
        added = [shape((rows, LANES), BF), shape((8, LANES), F32)]
    n_in, n_out = len(blocked) + len(slots), len(outs) + len(whole)

    def body(*refs):
        refs = list(refs)
        ins, refs = refs[:n_in], refs[n_in:]
        before, refs = refs[: len(extra)], refs[len(extra) :]
        out, refs = refs[:n_out], refs[n_out:]
        flown, refs = refs[: len(added)], refs[len(added) :]
        own, after = refs[: len(scratch)], refs[len(scratch) :]
        step = pl.program_id(0)
        if carried:
            flow = Flow(SHARES, *before, *flown, *after)
            flow.at_start(step)
        kernel(*ins, *out, *own)
        if carried:
            flow.at_end(step)

    nbytes = sum(b.size * b.dtype.itemsize for b in (*blocked, *slots, *outs, *whole))
    return pl.pallas_call(
        body,
        name=name,
        grid=(tokens // tb,),
        in_specs=[by_token(b.shape[1]) for b in blocked] + [pl.BlockSpec(memory_space=ANY)] * (len(slots) + len(extra)),
        out_specs=[by_token(o.shape[1]) for o in outs]
        + [pl.BlockSpec(o.shape, lambda i, k=len(o.shape): (0,) * k) for o in (*whole, *added)],
        scratch_shapes=list(scratch) + more,
        out_shape=[*outs, *whole, *added],
        input_output_aliases=aliases or {},
        compiler_params=params(collective_id=ident, has_side_effects=True) if carried else params(),
        cost_estimate=pl.CostEstimate(flops=flops, bytes_accessed=nbytes, transcendentals=0),
    )(*blocked, *slots, *extra)


def grads(width):
    return [jax.ShapeDtypeStruct((2, 15 * width // 4, LANES), BF)] * 2


def back_scratch(d, width, gu):
    tb = TOKENS_PER_STEP
    return ([VMEM((d, 2 * width), BF)] if gu else []) + [
        VMEM((width, d), BF), VMEM((d, 2 * width), F32), VMEM((d, width), F32), VMEM((width, d), F32),
        VMEM((d, tb), BF), VMEM((d, tb), BF), pltpu.SemaphoreType.DMA((2,)),
    ]


def forward_call(runs, first, last, name, x, y, slots):
    tokens, d = x.shape
    width, shape = 4 * units(runs), jax.ShapeDtypeStruct
    end = [shape((tokens, d), BF)] * 2 if last else [shape((tokens, d), F32)]
    return call(
        functools.partial(forward_kernel, runs, first, last), name, tokens, [x] if first else [x, y], slots,
        [shape((tokens, width), F32)] * 2 + end, [],
        [VMEM((d, 2 * width), BF), VMEM((width, d), BF), VMEM((TOKENS_PER_STEP, width), BF), pltpu.SemaphoreType.DMA((2,))],
        6 * tokens * d * width, aliases={} if first or last else {1: 2},
    )


def last_call(runs, first, last, name, a, dy, da, h, slots, carried=None, ident=None):
    tokens, d = a.shape
    width = 4 * units(runs)
    return call(
        functools.partial(last_kernel, runs, first, last), name, tokens,
        [a, dy] + ([] if first else [da]) + ([h] if last else []), slots,
        [jax.ShapeDtypeStruct((tokens, d), BF if last else F32)], grads(width),
        back_scratch(d, width, True) + [VMEM((TOKENS_PER_STEP, 2 * width), BF)],
        16 * tokens * d * width, aliases={} if first or last else {2: 0}, carried=carried, ident=ident,
    )


def back_call(runs, name, x, dh, gate, up, slots, carried=None, ident=None):
    tokens, d = x.shape
    width = 4 * units(runs)
    return call(
        functools.partial(first_back_kernel, runs), name, tokens, [x, dh, gate, up], slots, [], grads(width),
        back_scratch(d, width, False), 8 * tokens * d * width, carried=carried, ident=ident,
    )


def bench_forward(r, me, x, acc, slots, name):
    return forward_call(r, False, False, name, x, acc, slots)


def bench_last(r, me, x, acc, slots, name):
    return last_call(r, False, False, name, x, x, acc, None, slots)


def bench_back(r, me, x, g, slots, name):
    return back_call(r, name, x, x, g, g, slots)


def update_gu_kernel(factor_ref, *refs):
    packs, refs = refs[: 2 * len(CHUNKS)], refs[2 * len(CHUNKS) :]
    ins, outs, g_ref = refs[:6], refs[6:12], refs[12]
    for l in range(2):

        @pl.when(pl.program_id(0) == l)
        def _(l=l):
            for i in range(2):
                for runs, pack in zip(CHUNKS, packs[l * len(CHUNKS) : (l + 1) * len(CHUNKS)]):
                    tile = i * units(runs) // 32
                    for first, n in runs:
                        if n >= LANES:
                            for s in range(4):
                                for t in range(n // LANES):
                                    g_ref[i, :, pl.ds(s * 800 + first + t * LANES, LANES)] = pack[tile].astype(F32)
                                    tile += 1
                        else:
                            four = pack[tile].astype(F32)
                            for s in range(4):
                                g_ref[i, :, pl.ds(s * 800 + first, n)] = four[:, s * n : (s + 1) * n]

    for i in range(2):
        w, m, v = (r[0] for r in ins[3 * i : 3 * i + 3])
        g = g_ref[i] * factor_ref[0:1, 0:1]
        for o, value in zip(outs[3 * i : 3 * i + 3], adamw(w.astype(F32), m, v, g)):
            o[0] = value


def update_d_kernel(factor_ref, *refs):
    packs, (w_ref, m_ref, v_ref, wo, mo, vo) = refs[: 2 * len(CHUNKS)], refs[2 * len(CHUNKS) :]
    for l in range(2):

        @pl.when(pl.program_id(0) == l)
        def _(l=l):
            for runs, pack in zip(CHUNKS, packs[l * len(CHUNKS) : (l + 1) * len(CHUNKS)]):
                first, n = runs[0][0], units(runs)
                at = (0, pl.ds(first, n))
                row = pl.multiple_of(10 * n + pl.program_id(1) * n, 32)
                g = pack[pl.ds(row, n), :].astype(F32) * factor_ref[0:1, :]
                wo[at], mo[at], vo[at] = adamw(w_ref[at].astype(F32), m_ref[at], v_ref[at], g)


def adamw(w, m, v, g):
    m = 0.9 * m + 0.1 * g
    v = 0.95 * v + 0.05 * g * g
    step = m * lax.rsqrt(v + 1e-8) + 0.1 * w
    return (w - 0.02 * step).astype(BF), m, v


def solution(mesh):
    core = [(s, s ^ 1) for s in range(4)]
    along_x = [(s, s ^ 2) for s in range(4)]

    def gathered(block, before):
        if before is not None:
            block, _ = lax.optimization_barrier((block, before))
        far = lax.ppermute(block, "s", along_x)
        return block, lax.ppermute(block, "s", core), far, lax.ppermute(far, "s", core)

    def step(x, dy, w_gate, w_up, w_down, *moments):
        x, dy = x[0], dy[0]
        tokens, d = x.shape
        shape = jax.ShapeDtypeStruct
        n = len(CHUNKS)

        blocks = [pack(l, w_gate, w_up, w_down) for l in range(2)]

        order = list(reversed(range(n)))
        wanted = [(0, j) for j in order] + [(1, j) for j in range(n)]
        slots = {}

        def ask(k, before):
            if k < len(wanted):
                l, j = wanted[k]
                slots[l, j] = gathered(blocks[l][j], before)

        ask(0, None)
        ask(1, slots[wanted[0]][2])
        kept, y = {}, None
        for j in order:
            first, last = j == order[0], j == order[-1]
            gate, up, *y = forward_call(CHUNKS[j], first, last, f"forward0_{j}", x, None if first else y[0], slots[0, j])
            kept[j] = gate, up
            ask(wanted.index((0, j)) + 2, y[0])
        h, a = y

        every, squares, pending, da = [], [], None, None
        for j in range(n):
            first, last = j == 0, j == n - 1
            got = last_call(CHUNKS[j], first, last, f"layer1_{j}", a, dy, da, h, slots[1, j], pending, j)
            da, *pending, g, sq = *got, *((None, None) if first else ())
            ask(n + j + 2, da)
            every, squares = every + [g], squares + [sq]
        for j in range(n):
            *pending, g, sq = back_call(CHUNKS[j], f"back0_{j}", x, da, *kept[j], slots[0, j], pending, n + j)
            every, squares = every + [g], squares + [sq]
        every, squares = every[1:], squares[1:]
        count = 4 * (sum(g.size for g in every) + pending[0].size // 2)
        g, factor = tail_call(count, *pending, squares, 2 * n)
        every = every[n:] + [g] + every[:n]

        m, v = moments[:3], moments[3:]
        smem = pl.BlockSpec(memory_space=VMEM)
        rows, block = w_gate.shape[1], 32
        packs = [g.reshape(-1, rows, LANES) for g in every]

        def pack_spec(g, l):
            def index(i, k):
                return (0, jnp.where(i == l, k, 0 if l else rows // block - 1), 0)
            return pl.BlockSpec((2 * g.shape[0] // 3, block, LANES), index)

        gu_spec = pl.BlockSpec((1, block, w_gate.shape[2]), lambda i, k: (i, k, 0))
        gu_shapes = [shape(w_gate.shape, t) for t in (BF, F32, F32)] * 2
        out_g = pl.pallas_call(
            update_gu_kernel,
            name="update_gu",
            grid=(2, rows // block),
            in_specs=[smem] + [pack_spec(g, i // n) for i, g in enumerate(packs)] + [gu_spec] * 6,
            out_specs=[gu_spec] * 6,
            out_shape=gu_shapes,
            scratch_shapes=[VMEM((2, block, w_gate.shape[2]), F32)],
            compiler_params=pltpu.CompilerParams(vmem_limit_bytes=60 * 2**20),
        )(factor, *packs, w_gate, m[0], v[0], w_up, m[1], v[1])
        d_spec = pl.BlockSpec((1, w_down.shape[1], LANES), lambda i, k: (i, 0, k))
        out_d = pl.pallas_call(
            update_d_kernel,
            name="update_d",
            grid=(2, w_down.shape[2] // LANES),
            in_specs=[smem] + [pl.BlockSpec(g.shape, lambda i, k: (0, 0)) for g in every] + [d_spec] * 3,
            out_specs=[d_spec] * 3,
            out_shape=[shape(w_down.shape, t) for t in (BF, F32, F32)],
            compiler_params=pltpu.CompilerParams(vmem_limit_bytes=60 * 2**20),
        )(factor, *every, w_down, m[2], v[2])
        return tuple(one for k in range(3) for one in (out_g[k], out_g[3 + k], out_d[k]))

    states, cut = P(("rep", "r", "s"), None, None), P(None, "s", None)
    return jax.shard_map(
        step,
        mesh=mesh,
        in_specs=(states, states) + (cut,) * 9,
        out_specs=(P("rep", "s", None),) * 9,
        check_vma=False,
    )
```

```python
import functools

import jax
import jax.numpy as jnp
from jax import lax
from jax.experimental import pallas as pl
from jax.experimental.pallas import tpu as pltpu
from jax.sharding import PartitionSpec as P


BF, F32 = jnp.bfloat16, jnp.float32
LANES = 128
VMEM_BYTES = 60 * 2**20
TOKENS_PER_STEP = 512
CHUNKS = (((0, 256),), ((256, 256),), ((512, 128), (640, 32)), ((672, 128),))
VMEM = pltpu.VMEM
ANY = pl.ANY


def params(**kw):
    return pltpu.CompilerParams(vmem_limit_bytes=VMEM_BYTES, **kw)


def units(runs):
    return sum(n for _, n in runs)


def dot(a, b):
    return jnp.dot(a, b, preferred_element_type=F32)


def dot_nt(a, b):
    return lax.dot_general(a, b, (((1,), (1,)), ((), ())), preferred_element_type=F32)


def scale_of(wide):
    return lax.rsqrt(jnp.mean(wide * wide, -1, keepdims=True) + 1e-6)


def sigmoid(x):
    return 0.5 * jnp.tanh(0.5 * x) + 0.5


def pack_block(l, runs, gate_ref, up_ref, down_ref, out):
    rows, row = gate_ref.shape[1], 0
    for ref in (gate_ref, up_ref):
        for first, n in runs:
            parts = [ref[l, :, pl.ds(s * 800 + first, n)] for s in range(4)]
            parts = [jnp.concatenate(parts, -1)] if n < LANES else [p[:, t : t + LANES] for p in parts for t in range(0, n, LANES)]
            for part in parts:
                out[pl.ds(row, rows), :] = part
                row += rows
    first, n = runs[0][0], units(runs)
    for t in range(down_ref.shape[2] // LANES):
        out[pl.ds(row, n), :] = down_ref[l, pl.ds(first, n), pl.ds(t * LANES, LANES)]
        row += n


def greet(targets):
    barrier = pltpu.get_barrier_semaphore()
    for target in targets:
        pl.semaphore_signal(barrier, inc=1, device_id=target, device_id_type=pl.DeviceIdType.MESH)
    pl.semaphore_wait(barrier, len(targets))


class Fetch:
    def __init__(self, block, near, far, corner, send_sems, recv_sems):
        _, core, x, _ = partners(lax.axis_index("s"))
        self.targets = [{"s": x}, {"s": core}]
        self.ways = ((block, far, 0), (block, near, 1), (far, corner, 1))
        self.send_sems, self.recv_sems = send_sems, recv_sems

    def way(self, i):
        src, dst, target = self.ways[i]
        return pltpu.make_async_remote_copy(
            src_ref=src, dst_ref=dst, send_sem=self.send_sems.at[i], recv_sem=self.recv_sems.at[i],
            device_id=self.targets[target], device_id_type=pl.DeviceIdType.MESH,
        )

    def start(self):
        self.way(0).start()
        self.way(1).start()

    def forward(self):
        self.way(0).wait()
        self.way(2).start()

    def finish(self):
        self.way(1).wait()
        self.way(2).wait()


def fetch_scratch():
    return [pltpu.SemaphoreType.DMA((3,)), pltpu.SemaphoreType.DMA((3,))]


def open_kernel(wanted, gate_ref, up_ref, down_ref, *refs):
    blocks, (near, far, corner, send_sems, recv_sems) = refs[: len(wanted)], refs[len(wanted) :]
    fetching = Fetch(blocks[0], near, far, corner, send_sems, recv_sems)
    for i, (l, j) in enumerate(wanted):
        pack_block(l, CHUNKS[j], gate_ref, up_ref, down_ref, blocks[i])
        if i == 1:
            greet(fetching.targets)
            fetching.start()
    fetching.forward()
    fetching.finish()


def open_call(wanted, gate, up, down, ident):
    spec = lambda w: pl.BlockSpec(w.shape, lambda i: (0, 0, 0))
    shapes = [jax.ShapeDtypeStruct((15 * units(CHUNKS[j]), LANES), BF) for _, j in wanted]
    return pl.pallas_call(
        functools.partial(open_kernel, wanted),
        name="open",
        grid=(1,),
        in_specs=[spec(w) for w in (gate, up, down)],
        out_specs=[pl.BlockSpec(o.shape, lambda i: (0, 0)) for o in shapes] + [pl.BlockSpec(memory_space=pltpu.HBM)] * 3,
        out_shape=shapes + [shapes[0]] * 3,
        scratch_shapes=fetch_scratch(),
        compiler_params=params(collective_id=ident, has_side_effects=True),
    )(gate, up, down)


def partners(s):
    swap = lambda i: i + 1 - 2 * lax.rem(i, 2)
    far = lax.rem(s + 2, 4)
    return s, swap(s), far, swap(far)


def fetch(slots, wgu, wd, sems, runs):
    f = units(runs)
    tiles = 8 * f // LANES
    rows = 160
    copies = []
    for s, slot in zip(partners(lax.axis_index("s")), slots):
        if wgu is not None:
            at = pl.ds(pl.multiple_of(s * rows, 32), rows)
            for t in range(tiles):
                copies.append(pltpu.make_async_copy(slot.at[pl.ds(t * rows, rows)], wgu.at[at, pl.ds(t * LANES, LANES)], sems.at[0]))
        for t in range(5):
            row, place = tiles * rows + t * f, 0
            for _, n in runs:
                at = pl.ds(pl.multiple_of(place + s * n, 32), n)
                copies.append(pltpu.make_async_copy(slot.at[pl.ds(row, n)], wd.at[at, pl.ds(t * LANES, LANES)], sems.at[1]))
                row, place = row + n, place + 4 * n
    for copy in copies:
        copy.start()
    if wgu is not None:
        pltpu.make_async_copy(wgu, wgu, sems.at[0]).wait()
    pltpu.make_async_copy(wd, wd, sems.at[1]).wait()


def pieces(width):
    return [(c, min(512, width - c)) for c in range(0, width, 512)]


def deliver(acc_gu, acc_d, turned, keep, send, runs):
    f = units(runs)
    tiles, rows = 8 * f // LANES, 160
    turned[...] = acc_d[...].T
    for k, s in enumerate(partners(lax.axis_index("s"))):
        out = (send if k % 2 else keep).at[k // 2]
        at = pl.ds(pl.multiple_of(s * rows, 32), rows)
        for t in range(tiles):
            out[pl.ds(t * rows, rows), :] = acc_gu[at, pl.ds(t * LANES, LANES)].astype(BF)
        for t in range(5):
            row, place = tiles * rows + t * f, 0
            for _, n in runs:
                at_d = pl.ds(pl.multiple_of(place + s * n, 32), n)
                out[pl.ds(row, n), :] = turned[at_d, pl.ds(t * LANES, LANES)].astype(BF)
                row, place = row + n, place + 4 * n


def cuts(rows, shares):
    ends = [0]
    for share in shares:
        ends.append(ends[-1] + share)
    ends = [rows * e // ends[-1] // 16 * 16 for e in ends]
    return [(a, b - a) for a, b in zip(ends, ends[1:])]


class Flow:
    def targets(self):
        _, core, x, _ = partners(lax.axis_index("s"))
        _, z, y, _ = partners(lax.axis_index("r"))
        return [{"s": x}, {"r": y}, {"r": z}, {"s": core}]

    def remote(self, src, dst, sem, target):
        return pltpu.make_async_remote_copy(
            src_ref=src, dst_ref=dst, send_sem=self.send_sems.at[sem], recv_sem=self.recv_sems.at[sem],
            device_id=self.targets()[target], device_id_type=pl.DeviceIdType.MESH,
        )

    def rows(self, p):
        first, n = self.cuts[p]
        return [pl.ds(first + i, min(160, n - i)) for i in range(0, n, 160)]


class Near(Flow):
    def __init__(self, shares, keep, send, out, own, got, far, local_sem, send_sems, recv_sems):
        self.keep, self.send, self.out, self.own, self.got, self.far = keep, send, out, own, got, far
        self.local_sem, self.send_sems, self.recv_sems = local_sem, send_sems, recv_sems
        self.cuts = cuts(own.shape[1], shares)

    def local(self):
        return pltpu.make_async_copy(self.keep, self.own, self.local_sem)

    def core(self):
        return self.remote(self.send, self.got, 0, 3)

    def enter(self):
        self.local().start()
        self.core().start()

    def add_core(self):
        self.local().wait()
        self.core().wait()
        for p in range(len(self.cuts)):
            for at in self.rows(p):
                self.own[1, at, :] = (self.own[1, at, :].astype(F32) + self.got[1, at, :].astype(F32)).astype(BF)

    def hop(self, p):
        at = pl.ds(*self.cuts[p])
        return self.remote(self.own.at[1, at], self.far.at[at], 1 + p, 0)

    def add(self, p):
        self.hop(p).wait()
        for at in self.rows(p):
            total = self.own[0, at, :].astype(F32) + self.got[0, at, :].astype(F32) + self.far[at, :].astype(F32)
            self.out[at, :] = total.astype(BF)

    def at_start(self, step):
        pl.when(step == 0)(self.enter)

        @pl.when(step == 1)
        def _():
            for p in range(len(self.cuts)):
                self.hop(p).start()

    def at_end(self, step):
        pl.when(step == 0)(self.add_core)

        @pl.when(step == pl.num_programs(0) - 1)
        def _():
            for p in range(len(self.cuts)):
                self.add(p)


class Wide(Flow):
    def __init__(self, start, out, squares, own, far, local_sem, send_sems, recv_sems):
        self.begin, self.out, self.squares, self.own, self.far = start, out, squares, own, far
        self.local_sem, self.send_sems, self.recv_sems = local_sem, send_sems, recv_sems
        self.cuts = cuts(own.shape[0], (1, 1))

    def local(self):
        return pltpu.make_async_copy(self.begin, self.own, self.local_sem)

    def hop(self, stage, p):
        at = pl.ds(*self.cuts[p])
        return self.remote(self.own.at[at], self.far.at[stage, at], 2 * stage + p, 1 + (stage + p) % 2)

    def add(self, stage, p):
        self.hop(stage, p).wait()
        for at in self.rows(p):
            total = (self.own[at, :].astype(F32) + self.far[stage, at, :].astype(F32)).astype(BF)
            if stage:
                self.out[at, :] = total
                wide = total.astype(F32)
                self.squares[...] += jnp.sum((wide * wide).reshape(-1, 8, LANES), 0)
            else:
                self.own[at, :] = total

    def start(self, stage):
        for p in range(len(self.cuts)):
            self.hop(stage, p).start()

    def end(self, stage):
        for p in range(len(self.cuts)):
            self.add(stage, p)

    def at_start(self, step):
        @pl.when(step == 0)
        def _():
            self.squares[...] = jnp.zeros_like(self.squares)
            self.local().start()

        for stage, at in enumerate(STARTS):
            pl.when(step == at)(functools.partial(self.start, stage))

    def at_end(self, step):
        pl.when(step == 0)(lambda: self.local().wait())
        for stage, at in enumerate(ENDS):
            pl.when(step == at)(functools.partial(self.end, stage))


STARTS, ENDS = (1, 4), (3, 7)


def near_scratch(rows, shares):
    sems = pltpu.SemaphoreType.DMA((1 + len(shares),))
    return [VMEM((2, rows, LANES), BF), VMEM((2, rows, LANES), BF), VMEM((rows, LANES), BF), pltpu.SemaphoreType.DMA, sems, sems]


def wide_scratch(rows):
    sems = pltpu.SemaphoreType.DMA((4,))
    return [VMEM((rows, LANES), BF), VMEM((2, rows, LANES), BF), pltpu.SemaphoreType.DMA, sems, sems]


def tail_kernel(count, parts, keep, send, half, *refs):
    sums, (out, out_before, factor_ref, *scratch) = refs[:parts], refs[parts:]
    near, before, wide = scratch[:6], scratch[6:11], scratch[11:16]
    total, squares, theirs, s_sems, r_sems = scratch[16:]
    near = Near((1, 1), keep, send, total, *near)
    before = Wide(half, out_before, squares, *before)
    wide = Wide(None, out, squares, *wide)
    squares[...] = sums[0][...]
    for part in sums[1:]:
        squares[...] += part[...]
    greet(near.targets())
    near.enter()
    before.local().start()
    before.local().wait()
    before.start(0)
    near.add_core()
    for p in range(len(near.cuts)):
        near.hop(p).start()
    before.end(0)
    before.start(1)
    for p in range(len(near.cuts)):
        near.add(p)
        for at in near.rows(p):
            wide.own[at, :] = total[at, :]
        wide.hop(0, p).start()
    before.end(1)
    wide.end(0)
    wide.start(1)
    wide.end(1)
    targets = near.targets()
    for i, target in enumerate((3, 0)):
        copy = pltpu.make_async_remote_copy(
            src_ref=squares.at[...] if i == 0 else theirs.at[2], dst_ref=theirs.at[i], send_sem=s_sems.at[i], recv_sem=r_sems.at[i],
            device_id=targets[target], device_id_type=pl.DeviceIdType.MESH,
        )
        copy.start()
        copy.wait()
        if i == 0:
            theirs[2] = squares[...] + theirs[0]
        else:
            theirs[3] = theirs[2] + theirs[1]
    every = jnp.sum(theirs[3])
    factor_ref[...] = jnp.minimum(1.0, 0.5 * lax.rsqrt(jnp.full(factor_ref.shape, every, F32) / count + 1e-30))


def tail_call(count, keep, send, half, sums, ident):
    rows, before = keep.shape[1], half.shape[0]
    vmem = pl.BlockSpec(memory_space=VMEM)
    shape = jax.ShapeDtypeStruct
    return pl.pallas_call(
        functools.partial(tail_kernel, count, len(sums)),
        name="tail",
        in_specs=[pl.BlockSpec(memory_space=ANY)] * 3 + [vmem] * len(sums),
        out_specs=[vmem] * 3,
        out_shape=[shape((rows, LANES), BF), shape((before, LANES), BF), shape((8, LANES), F32)],
        scratch_shapes=near_scratch(rows, (1, 1)) + wide_scratch(before) + wide_scratch(rows)
        + [VMEM((rows, LANES), BF), VMEM((8, LANES), F32), VMEM((4, 8, LANES), F32), pltpu.SemaphoreType.DMA((2,)), pltpu.SemaphoreType.DMA((2,))],
        compiler_params=params(collective_id=ident, has_side_effects=True),
    )(keep, send, half, *sums)


def forward_kernel(runs, first, last, *refs):
    refs = list(refs)
    x_ref = refs.pop(0)
    y_in = None if first else refs.pop(0)
    slots = [refs.pop(0) for _ in range(4)]
    gate_ref, up_ref = refs.pop(0), refs.pop(0)
    outs = [refs.pop(0) for _ in range(2 if last else 1)]
    wgu, wd, prod_ref, sems = refs
    width = 4 * units(runs)

    @pl.when(pl.program_id(0) == 0)
    def _():
        fetch(slots, wgu, wd, sems, runs)

    wide = x_ref[...].astype(F32)
    a = (wide * scale_of(wide)).astype(BF)
    for c, n in pieces(width):
        g = dot(a, wgu[:, pl.ds(c, n)])
        u = dot(a, wgu[:, pl.ds(width + c, n)])
        gate_ref[:, pl.ds(c, n)] = g
        up_ref[:, pl.ds(c, n)] = u
        prod_ref[:, pl.ds(c, n)] = (g * sigmoid(g) * u).astype(BF)
    y = dot(prod_ref[...], wd[...])
    if not first:
        y = y + y_in[...]
    if last:
        h = (wide + y.astype(BF).astype(F32)).astype(BF)
        outs[0][...] = h
        wide = h.astype(F32)
        outs[1][...] = (wide * scale_of(wide)).astype(BF)
    else:
        outs[0][...] = y


def swiglu_back(g, u, dp):
    dp = dp.astype(BF).astype(F32)
    sig = sigmoid(g)
    act = g * sig
    return (act * u).astype(BF), (dp * u * (sig + act * (1.0 - sig))).astype(BF), (dp * act).astype(BF)


def last_kernel(runs, first, last, *refs):
    refs = list(refs)
    a_ref, dy_ref = refs.pop(0), refs.pop(0)
    da_in = None if first else refs.pop(0)
    h_ref = refs.pop(0) if last else None
    slots = [refs.pop(0) for _ in range(4)]
    out_ref, keep, send = refs.pop(0), refs.pop(0), refs.pop(0)
    wgu, wd, acc_gu, acc_d, turned, at_ref, dyt_ref, sems, dcat = refs
    width = 4 * units(runs)

    @pl.when(pl.program_id(0) == 0)
    def _():
        acc_gu[...] = jnp.zeros_like(acc_gu)
        acc_d[...] = jnp.zeros_like(acc_d)
        fetch(slots, wgu, wd, sems, runs)

    a, dy = a_ref[...], dy_ref[...]
    at_ref[...] = a.T
    dyt_ref[...] = dy.T
    for c, n in pieces(width):
        g = dot(a, wgu[:, pl.ds(c, n)])
        u = dot(a, wgu[:, pl.ds(width + c, n)])
        dp = dot_nt(dy, wd[pl.ds(c, n), :])
        prod, dg, du = swiglu_back(g, u, dp)
        dcat[:, pl.ds(c, n)], dcat[:, pl.ds(width + c, n)] = dg, du
        acc_d[:, pl.ds(c, n)] += dot(dyt_ref[...], prod)
        acc_gu[:, pl.ds(c, n)] += dot(at_ref[...], dg)
        acc_gu[:, pl.ds(width + c, n)] += dot(at_ref[...], du)
    da = dot_nt(dcat[...], wgu[...])
    if not first:
        da = da + da_in[...]
    if last:
        da = da.astype(BF).astype(F32)
        wide = h_ref[...].astype(F32)
        scale = scale_of(wide)
        by_scale = jnp.mean(da * wide, -1, keepdims=True)
        by_h = (da * scale - wide * (scale * scale * scale * by_scale)).astype(BF)
        out_ref[...] = (dy.astype(F32) + by_h.astype(F32)).astype(BF)
    else:
        out_ref[...] = da

    @pl.when(pl.program_id(0) == pl.num_programs(0) - 1)
    def _():
        deliver(acc_gu, acc_d, turned, keep, send, runs)


def first_back_kernel(runs, *refs):
    x_ref, dh_ref, gate_ref, up_ref, *refs = refs
    slots, (keep, send, wd, acc_gu, acc_d, turned, at_ref, dht_ref, sems) = refs[:4], refs[4:]
    width = 4 * units(runs)

    @pl.when(pl.program_id(0) == 0)
    def _():
        acc_gu[...] = jnp.zeros_like(acc_gu)
        acc_d[...] = jnp.zeros_like(acc_d)
        fetch(slots, None, wd, sems, runs)

    wide = x_ref[...].astype(F32)
    a = (wide * scale_of(wide)).astype(BF)
    dh = dh_ref[...]
    at_ref[...] = a.T
    dht_ref[...] = dh.T
    for c, n in pieces(width):
        dp = dot_nt(dh, wd[pl.ds(c, n), :])
        g, u = gate_ref[:, pl.ds(c, n)], up_ref[:, pl.ds(c, n)]
        prod, dg, du = swiglu_back(g, u, dp)
        acc_d[:, pl.ds(c, n)] += dot(dht_ref[...], prod)
        acc_gu[:, pl.ds(c, n)] += dot(at_ref[...], dg)
        acc_gu[:, pl.ds(width + c, n)] += dot(at_ref[...], du)

    @pl.when(pl.program_id(0) == pl.num_programs(0) - 1)
    def _():
        deliver(acc_gu, acc_d, turned, keep, send, runs)


def call(kernel, name, tokens, blocked, slots, outs, whole, scratch, flops, aliases=None, carried=None, half=None, wanted=None, ident=None):
    tb = TOKENS_PER_STEP
    by_token = lambda width: pl.BlockSpec((tb, width), lambda i: (i, 0))
    shape = jax.ShapeDtypeStruct
    extra, added, more, flows = [], [], [], []
    if carried:
        rows = carried[0].shape[1]
        flows.append((functools.partial(Near, (1,)), len(extra), len(added), len(more), 2, 1, 6))
        extra, more = extra + list(carried), more + near_scratch(rows, (1,))
        added = added + [shape((rows, LANES), BF)]
    if half is not None:
        flows.append((Wide, len(extra), len(added), len(more), 1, 2, 5))
        extra, more = extra + [half], more + wide_scratch(half.shape[0])
        added = added + [shape(half.shape, BF), shape((8, LANES), F32)]
    n_in, n_out = len(blocked) + len(slots), len(outs) + len(whole)
    blocks = [] if wanted is None else [wanted]
    fetched = [shape(wanted.shape, BF)] * 3 if blocks else []
    sems = fetch_scratch() if blocks else []

    def body(*refs):
        refs = list(refs)
        ins, refs = refs[:n_in], refs[n_in:]
        before, refs = refs[: len(extra)], refs[len(extra) :]
        block, refs = refs[: len(blocks)], refs[len(blocks) :]
        out, refs = refs[:n_out], refs[n_out:]
        flown, refs = refs[: len(added)], refs[len(added) :]
        there, refs = refs[: len(fetched)], refs[len(fetched) :]
        own, refs = refs[: len(scratch)], refs[len(scratch) :]
        after, sems = refs[: len(more)], refs[len(more) :]
        step = pl.program_id(0)
        going = [make(*before[i : i + a], *flown[j : j + b], *after[k : k + c]) for make, i, j, k, a, b, c in flows]
        if going:
            pl.when(step == 0)(lambda: greet(going[0].targets()))
        for flow in going:
            flow.at_start(step)
        if blocks:
            fetching = Fetch(*block, *there, *sems)

            @pl.when(step == 0)
            def _():
                if not going:
                    greet(fetching.targets)
                fetching.start()

        kernel(*ins, *out, *own)
        for flow in reversed(going):
            flow.at_end(step)
        if blocks:
            pl.when(step == pl.num_programs(0) - 2)(fetching.forward)
            pl.when(step == pl.num_programs(0) - 1)(fetching.finish)

    nbytes = sum(b.size * b.dtype.itemsize for b in (*blocked, *slots, *outs, *whole))
    return pl.pallas_call(
        body,
        name=name,
        grid=(tokens // tb,),
        in_specs=[by_token(b.shape[1]) for b in blocked] + [pl.BlockSpec(memory_space=ANY)] * (len(slots) + len(extra) + len(blocks)),
        out_specs=[by_token(o.shape[1]) for o in outs]
        + [pl.BlockSpec(o.shape, lambda i, k=len(o.shape): (0,) * k) for o in (*whole, *added)]
        + [pl.BlockSpec(memory_space=pltpu.HBM)] * len(fetched),
        scratch_shapes=list(scratch) + more + sems,
        out_shape=[*outs, *whole, *added, *fetched],
        input_output_aliases=aliases or {},
        compiler_params=params(collective_id=ident, has_side_effects=True) if flows or blocks else params(),
        cost_estimate=pl.CostEstimate(flops=flops, bytes_accessed=nbytes, transcendentals=0),
    )(*blocked, *slots, *extra, *blocks)


def grads(width):
    return [jax.ShapeDtypeStruct((2, 15 * width // 4, LANES), BF)] * 2


def back_scratch(d, width, gu):
    tb = TOKENS_PER_STEP
    return ([VMEM((d, 2 * width), BF)] if gu else []) + [
        VMEM((width, d), BF), VMEM((d, 2 * width), F32), VMEM((d, width), F32), VMEM((width, d), F32),
        VMEM((d, tb), BF), VMEM((d, tb), BF), pltpu.SemaphoreType.DMA((2,)),
    ]


def forward_call(runs, first, last, name, x, y, slots, wanted=None, ident=None):
    tokens, d = x.shape
    width, shape = 4 * units(runs), jax.ShapeDtypeStruct
    end = [shape((tokens, d), BF)] * 2 if last else [shape((tokens, d), F32)]
    return call(
        functools.partial(forward_kernel, runs, first, last), name, tokens, [x] if first else [x, y], slots,
        [shape((tokens, width), F32)] * 2 + end, [],
        [VMEM((d, 2 * width), BF), VMEM((width, d), BF), VMEM((TOKENS_PER_STEP, width), BF), pltpu.SemaphoreType.DMA((2,))],
        6 * tokens * d * width, aliases={} if first or last else {1: 2}, wanted=wanted, ident=ident,
    )


def last_call(runs, first, last, name, a, dy, da, h, slots, carried=None, half=None, wanted=None, ident=None):
    tokens, d = a.shape
    width = 4 * units(runs)
    return call(
        functools.partial(last_kernel, runs, first, last), name, tokens,
        [a, dy] + ([] if first else [da]) + ([h] if last else []), slots,
        [jax.ShapeDtypeStruct((tokens, d), BF if last else F32)], grads(width),
        back_scratch(d, width, True) + [VMEM((TOKENS_PER_STEP, 2 * width), BF)],
        16 * tokens * d * width, aliases={} if first or last else {2: 0}, carried=carried, half=half, wanted=wanted, ident=ident,
    )


def back_call(runs, name, x, dh, gate, up, slots, carried=None, half=None, ident=None):
    tokens, d = x.shape
    width = 4 * units(runs)
    return call(
        functools.partial(first_back_kernel, runs), name, tokens, [x, dh, gate, up], slots, [], grads(width),
        back_scratch(d, width, False), 8 * tokens * d * width, carried=carried, half=half, ident=ident,
    )


def update_kernel(factor_ref, *refs):
    n = 2 * len(CHUNKS)
    blocks, packs, ins, outs, g_ref = refs[:n], refs[n : 2 * n], refs[2 * n : 2 * n + 9], refs[2 * n + 9 : 2 * n + 18], refs[2 * n + 18]
    w_down, m_down, v_down = ins[6:]
    for l in range(2):

        @pl.when(pl.program_id(0) == l)
        def _(l=l):
            for runs, block, pack in zip(CHUNKS, blocks[l * n // 2 :], packs[l * n // 2 :]):
                for i in range(2):
                    tile = i * units(runs) // 32
                    for first, size in runs:
                        if size >= LANES:
                            for s in range(4):
                                for t in range(size // LANES):
                                    g_ref[i, :, pl.ds(s * 800 + first + t * LANES, LANES)] = block[tile].astype(F32)
                                    tile += 1
                        else:
                            four = block[tile].astype(F32)
                            for s in range(4):
                                g_ref[i, :, pl.ds(s * 800 + first, size)] = four[:, s * size : (s + 1) * size]
                first, size = runs[0][0], units(runs)
                for t in range(5):

                    @pl.when(pl.program_id(1) == t)
                    def _(t=t, first=first, size=size, pack=pack):
                        at = (0, pl.ds(first, size), pl.ds(t * LANES, LANES))
                        g = pack[pl.ds((10 + t) * size, size), :].astype(F32) * factor_ref[0:1, :]
                        for o, value in zip(outs[6:], adamw(w_down[at].astype(F32), m_down[at], v_down[at], g)):
                            o[at] = value

    for i in range(2):
        w, m, v = (r[0] for r in ins[3 * i : 3 * i + 3])
        g = g_ref[i] * factor_ref[0:1, 0:1]
        for o, value in zip(outs[3 * i : 3 * i + 3], adamw(w.astype(F32), m, v, g)):
            o[0] = value


def adamw(w, m, v, g):
    m = 0.9 * m + 0.1 * g
    v = 0.95 * v + 0.05 * g * g
    step = m * lax.rsqrt(v + 1e-8) + 0.1 * w
    return (w - 0.02 * step).astype(BF), m, v


def solution(mesh):
    def step(x, dy, w_gate, w_up, w_down, *moments):
        x, dy = x[0], dy[0]
        tokens, d = x.shape
        shape = jax.ShapeDtypeStruct
        n = len(CHUNKS)

        order = list(reversed(range(n)))
        wanted = [(0, j) for j in order] + [(1, j) for j in range(n)]
        got = open_call(wanted, w_gate, w_up, w_down, 0)
        own, there = got[: 2 * n], got[2 * n :]
        slots = {wanted[0]: (own[0], *there)}
        kept, y = {}, None
        for k, j in enumerate(order):
            gate, up, *got = forward_call(CHUNKS[j], k == 0, k == n - 1, f"forward0_{j}", x, y, slots[0, j], own[k + 1], 1 + k)
            kept[j] = gate, up
            y, there = got[0], got[-3:]
            slots[wanted[k + 1]] = (own[k + 1], *there)
        h, a = got[:2]

        every, squares, pair, half, da = [], [], None, None, None
        for l, j in [(1, j) for j in range(n)] + [(0, j) for j in range(n)]:
            more = None
            if l:
                more = None if j == n - 1 else own[n + j + 1]
                got = last_call(CHUNKS[j], j == 0, j == n - 1, f"layer1_{j}", a, dy, da, h, slots[1, j], pair, half, more, 1 + n + j)
                da, *got = got
            else:
                got = back_call(CHUNKS[j], f"back0_{j}", x, da, *kept[j], slots[0, j], pair, half, 1 + 2 * n + j)
            new, got = got[:2], list(got[2:])
            new_half = got.pop(0) if pair else None
            if half is not None:
                every, squares = every + [got.pop(0)], squares + [got.pop(0)]
            if more is not None:
                slots[1, j + 1] = (more, *got)
            pair, half = new, new_half
        count = 4 * (sum(g.size for g in every) + half.size + pair[0].size // 2)
        g, before, factor = tail_call(count, *pair, half, squares, 1 + 3 * n)
        every = every[n:] + [before, g] + every[:n]

        m, v = moments[:3], moments[3:]
        smem = pl.BlockSpec(memory_space=VMEM)
        rows, block = w_gate.shape[1], 32
        packs = [g.reshape(-1, rows, LANES) for g in every]

        def pack_spec(g, l):
            def index(i, k):
                return (0, jnp.where(i == l, k, 0 if l else rows // block - 1), 0)
            return pl.BlockSpec((2 * g.shape[0] // 3, block, LANES), index)

        gu_spec = pl.BlockSpec((1, block, w_gate.shape[2]), lambda i, k: (i, k, 0))
        gu_shapes = [shape(w_gate.shape, t) for t in (BF, F32, F32)] * 2
        d_spec = pl.BlockSpec((1, *w_down.shape[1:]), lambda i, k: (i, 0, 0))
        out = pl.pallas_call(
            update_kernel,
            name="update",
            grid=(2, rows // block),
            in_specs=[smem]
            + [pack_spec(g, i // n) for i, g in enumerate(packs)]
            + [pl.BlockSpec(g.shape, lambda i, k: (0, 0)) for g in every]
            + [gu_spec] * 6 + [d_spec] * 3,
            out_specs=[gu_spec] * 6 + [d_spec] * 3,
            out_shape=gu_shapes + [shape(w_down.shape, t) for t in (BF, F32, F32)],
            scratch_shapes=[VMEM((2, block, w_gate.shape[2]), F32)],
            compiler_params=params(),
        )(factor, *packs, *every, w_gate, m[0], v[0], w_up, m[1], v[1], w_down, m[2], v[2])
        return tuple(out[3 * i + k] for k in range(3) for i in range(3))

    states, cut = P(("rep", "r", "s"), None, None), P(None, "s", None)
    return jax.shard_map(
        step,
        mesh=mesh,
        in_specs=(states, states) + (cut,) * 9,
        out_specs=(P("rep", "s", None),) * 9,
        check_vma=False,
    )
```

```python
import functools

import jax
import jax.numpy as jnp
from jax import lax
from jax.experimental import pallas as pl
from jax.experimental.pallas import tpu as pltpu
from jax.sharding import PartitionSpec as P


BF, F32 = jnp.bfloat16, jnp.float32
LANES = 128
VMEM_BYTES = 60 * 2**20
TOKENS_PER_STEP = 512
CHUNKS = (((0, 256),), ((256, 256),), ((512, 128), (640, 32)), ((672, 128),))
VMEM = pltpu.VMEM
ANY = pl.ANY


def params(**kw):
    return pltpu.CompilerParams(vmem_limit_bytes=VMEM_BYTES, **kw)


def units(runs):
    return sum(n for _, n in runs)


def dot(a, b):
    return jnp.dot(a, b, preferred_element_type=F32)


def dot_nt(a, b):
    return lax.dot_general(a, b, (((1,), (1,)), ((), ())), preferred_element_type=F32)


def scale_of(wide):
    return lax.rsqrt(jnp.mean(wide * wide, -1, keepdims=True) + 1e-6)


def sigmoid(x):
    return 0.5 * jnp.tanh(0.5 * x) + 0.5


def pack_block(l, runs, gate_ref, up_ref, down_ref, out):
    rows, row = gate_ref.shape[1], 0
    for ref in (gate_ref, up_ref):
        for first, n in runs:
            parts = [ref[l, :, pl.ds(s * 800 + first, n)] for s in range(4)]
            parts = [jnp.concatenate(parts, -1)] if n < LANES else [p[:, t : t + LANES] for p in parts for t in range(0, n, LANES)]
            for part in parts:
                out[pl.ds(row, rows), :] = part
                row += rows
    first, n = runs[0][0], units(runs)
    for t in range(down_ref.shape[2] // LANES):
        out[pl.ds(row, n), :] = down_ref[l, pl.ds(first, n), pl.ds(t * LANES, LANES)]
        row += n


def greet(targets):
    barrier = pltpu.get_barrier_semaphore()
    for target in targets:
        pl.semaphore_signal(barrier, inc=1, device_id=target, device_id_type=pl.DeviceIdType.MESH)
    pl.semaphore_wait(barrier, len(targets))


class Fetch:
    def __init__(self, block, near, far, corner, send_sems, recv_sems):
        _, core, x, _ = partners(lax.axis_index("s"))
        self.partners = [{"s": x}, {"s": core}]
        self.ways = ((block, far, 0), (block, near, 1), (far, corner, 1))
        self.send_sems, self.recv_sems = send_sems, recv_sems

    def targets(self):
        return self.partners

    def way(self, i):
        src, dst, target = self.ways[i]
        return pltpu.make_async_remote_copy(
            src_ref=src, dst_ref=dst, send_sem=self.send_sems.at[i], recv_sem=self.recv_sems.at[i],
            device_id=self.partners[target], device_id_type=pl.DeviceIdType.MESH,
        )

    def start(self):
        self.way(0).start()
        self.way(1).start()

    def forward(self):
        self.way(0).wait()
        self.way(2).start()

    def finish(self):
        self.way(1).wait()
        self.way(2).wait()


def fetch_scratch():
    return [pltpu.SemaphoreType.DMA((3,)), pltpu.SemaphoreType.DMA((3,))]


def open_kernel(wanted, gate_ref, up_ref, down_ref, *refs):
    blocks, (near, far, corner, send_sems, recv_sems) = refs[: len(wanted)], refs[len(wanted) :]
    fetching = Fetch(blocks[0], near, far, corner, send_sems, recv_sems)
    for i, (l, j) in enumerate(wanted):
        pack_block(l, CHUNKS[j], gate_ref, up_ref, down_ref, blocks[i])
        if i == 1:
            greet(fetching.targets())
            fetching.start()
    fetching.forward()
    fetching.finish()


def open_call(wanted, gate, up, down, ident):
    spec = lambda w: pl.BlockSpec(w.shape, lambda i: (0, 0, 0))
    shapes = [jax.ShapeDtypeStruct((15 * units(CHUNKS[j]), LANES), BF) for _, j in wanted]
    return pl.pallas_call(
        functools.partial(open_kernel, wanted),
        name="open",
        grid=(1,),
        in_specs=[spec(w) for w in (gate, up, down)],
        out_specs=[pl.BlockSpec(o.shape, lambda i: (0, 0)) for o in shapes] + [pl.BlockSpec(memory_space=pltpu.HBM)] * 3,
        out_shape=shapes + [shapes[0]] * 3,
        scratch_shapes=fetch_scratch(),
        compiler_params=params(collective_id=ident, has_side_effects=True),
    )(gate, up, down)


def partners(s):
    swap = lambda i: i + 1 - 2 * lax.rem(i, 2)
    far = lax.rem(s + 2, 4)
    return s, swap(s), far, swap(far)


def fetch(slots, wgu, wd, sems, runs, meanwhile):
    f = units(runs)
    tiles = 8 * f // LANES
    rows = 160
    copies = []
    for s, slot in zip(partners(lax.axis_index("s")), slots):
        if wgu is not None:
            at = pl.ds(pl.multiple_of(s * rows, 32), rows)
            for t in range(tiles):
                copies.append(pltpu.make_async_copy(slot.at[pl.ds(t * rows, rows)], wgu.at[at, pl.ds(t * LANES, LANES)], sems.at[0]))
        for t in range(5):
            row, place = tiles * rows + t * f, 0
            for _, n in runs:
                at = pl.ds(pl.multiple_of(place + s * n, 32), n)
                copies.append(pltpu.make_async_copy(slot.at[pl.ds(row, n)], wd.at[at, pl.ds(t * LANES, LANES)], sems.at[1]))
                row, place = row + n, place + 4 * n
    for copy in copies:
        copy.start()
    meanwhile()
    if wgu is not None:
        pltpu.make_async_copy(wgu, wgu, sems.at[0]).wait()
    pltpu.make_async_copy(wd, wd, sems.at[1]).wait()


def pieces(width):
    return [(c, min(512, width - c)) for c in range(0, width, 512)]


def deliver(acc_gu, acc_d, turned, keep, send, runs):
    f = units(runs)
    tiles, rows = 8 * f // LANES, 160
    turned[...] = acc_d[...].astype(BF).T
    for k, s in enumerate(partners(lax.axis_index("s"))):
        out = (send if k % 2 else keep).at[k // 2]
        at = pl.ds(pl.multiple_of(s * rows, 32), rows)
        for t in range(tiles):
            out[pl.ds(t * rows, rows), :] = acc_gu[at, pl.ds(t * LANES, LANES)].astype(BF)
        for t in range(5):
            row, place = tiles * rows + t * f, 0
            for _, n in runs:
                at_d = pl.ds(pl.multiple_of(place + s * n, 32), n)
                out[pl.ds(row, n), :] = turned[at_d, pl.ds(t * LANES, LANES)]
                row, place = row + n, place + 4 * n


def cuts(rows, shares):
    ends = [0]
    for share in shares:
        ends.append(ends[-1] + share)
    ends = [rows * e // ends[-1] // 16 * 16 for e in ends]
    return [(a, b - a) for a, b in zip(ends, ends[1:])]


class Flow:
    def targets(self):
        _, core, x, _ = partners(lax.axis_index("s"))
        _, z, y, _ = partners(lax.axis_index("r"))
        return [{"s": x}, {"r": y}, {"r": z}, {"s": core}]

    def remote(self, src, dst, sem, target):
        return pltpu.make_async_remote_copy(
            src_ref=src, dst_ref=dst, send_sem=self.send_sems.at[sem], recv_sem=self.recv_sems.at[sem],
            device_id=self.targets()[target], device_id_type=pl.DeviceIdType.MESH,
        )

    def rows(self, p):
        first, n = self.cuts[p]
        return [pl.ds(first + i, min(160, n - i)) for i in range(0, n, 160)]


class Near(Flow):
    def __init__(self, shares, keep, send, out, own, got, far, local_sem, send_sems, recv_sems):
        self.keep, self.send, self.out, self.own, self.got, self.far = keep, send, out, own, got, far
        self.local_sem, self.send_sems, self.recv_sems = local_sem, send_sems, recv_sems
        self.cuts = cuts(own.shape[1], shares)

    def local(self):
        return pltpu.make_async_copy(self.keep, self.own, self.local_sem)

    def core(self):
        return self.remote(self.send, self.got, 0, 3)

    def enter(self):
        self.local().start()
        self.core().start()

    def add_core(self):
        self.local().wait()
        self.core().wait()
        for p in range(len(self.cuts)):
            for at in self.rows(p):
                self.own[1, at, :] = (self.own[1, at, :].astype(F32) + self.got[1, at, :].astype(F32)).astype(BF)

    def hop(self, p):
        at = pl.ds(*self.cuts[p])
        return self.remote(self.own.at[1, at], self.far.at[at], 1 + p, 0)

    def add(self, p):
        self.hop(p).wait()
        for at in self.rows(p):
            total = self.own[0, at, :].astype(F32) + self.got[0, at, :].astype(F32) + self.far[at, :].astype(F32)
            self.out[at, :] = total.astype(BF)

    def at_start(self, step):
        @pl.when(step == 1)
        def _():
            for p in range(len(self.cuts)):
                self.hop(p).start()

    def at_end(self, step):
        pl.when(step == 0)(self.add_core)

        @pl.when(step == pl.num_programs(0) - 1)
        def _():
            for p in range(len(self.cuts)):
                self.add(p)


class Wide(Flow):
    def __init__(self, start, out, squares, own, far, local_sem, send_sems, recv_sems):
        self.begin, self.out, self.squares, self.own, self.far = start, out, squares, own, far
        self.local_sem, self.send_sems, self.recv_sems = local_sem, send_sems, recv_sems
        self.cuts = cuts(own.shape[0], (1, 1))

    def local(self):
        return pltpu.make_async_copy(self.begin, self.own, self.local_sem)

    def hop(self, stage, p):
        at = pl.ds(*self.cuts[p])
        return self.remote(self.own.at[at], self.far.at[stage, at], 2 * stage + p, 1 + (stage + p) % 2)

    def add(self, stage, p):
        self.hop(stage, p).wait()
        for at in self.rows(p):
            total = (self.own[at, :].astype(F32) + self.far[stage, at, :].astype(F32)).astype(BF)
            if stage:
                self.out[at, :] = total
                wide = total.astype(F32)
                self.squares[...] += jnp.sum((wide * wide).reshape(-1, 8, LANES), 0)
            else:
                self.own[at, :] = total

    def enter(self):
        self.squares[...] = jnp.zeros_like(self.squares)
        self.local().start()

    def start(self, stage):
        for p in range(len(self.cuts)):
            self.hop(stage, p).start()

    def end(self, stage):
        for p in range(len(self.cuts)):
            self.add(stage, p)

    def at_start(self, step):
        for stage, at in enumerate(STARTS):
            pl.when(step == at)(functools.partial(self.start, stage))

    def at_end(self, step):
        pl.when(step == 0)(lambda: self.local().wait())
        for stage, at in enumerate(ENDS):
            pl.when(step == at)(functools.partial(self.end, stage))


STARTS, ENDS = (1, 4), (3, 7)


def near_scratch(rows, shares):
    sems = pltpu.SemaphoreType.DMA((1 + len(shares),))
    return [VMEM((2, rows, LANES), BF), VMEM((2, rows, LANES), BF), VMEM((rows, LANES), BF), pltpu.SemaphoreType.DMA, sems, sems]


def wide_scratch(rows):
    sems = pltpu.SemaphoreType.DMA((4,))
    return [VMEM((rows, LANES), BF), VMEM((2, rows, LANES), BF), pltpu.SemaphoreType.DMA, sems, sems]


def tail_kernel(count, parts, keep, send, half, *refs):
    sums, (out, out_before, factor_ref, *scratch) = refs[:parts], refs[parts:]
    near, before, wide = scratch[:6], scratch[6:11], scratch[11:16]
    total, squares, theirs, s_sems, r_sems = scratch[16:]
    near = Near((1, 1), keep, send, total, *near)
    before = Wide(half, out_before, squares, *before)
    wide = Wide(None, out, squares, *wide)
    squares[...] = sums[0][...]
    for part in sums[1:]:
        squares[...] += part[...]
    greet(near.targets())
    near.enter()
    before.local().start()
    before.local().wait()
    before.start(0)
    near.add_core()
    for p in range(len(near.cuts)):
        near.hop(p).start()
    before.end(0)
    before.start(1)
    for p in range(len(near.cuts)):
        near.add(p)
        for at in near.rows(p):
            wide.own[at, :] = total[at, :]
        wide.hop(0, p).start()
    before.end(1)
    wide.end(0)
    wide.start(1)
    wide.end(1)
    targets = near.targets()
    for i, target in enumerate((3, 0)):
        copy = pltpu.make_async_remote_copy(
            src_ref=squares.at[...] if i == 0 else theirs.at[2], dst_ref=theirs.at[i], send_sem=s_sems.at[i], recv_sem=r_sems.at[i],
            device_id=targets[target], device_id_type=pl.DeviceIdType.MESH,
        )
        copy.start()
        copy.wait()
        if i == 0:
            theirs[2] = squares[...] + theirs[0]
        else:
            theirs[3] = theirs[2] + theirs[1]
    every = jnp.sum(theirs[3])
    factor_ref[...] = jnp.minimum(1.0, 0.5 * lax.rsqrt(jnp.full(factor_ref.shape, every, F32) / count + 1e-30))


def tail_call(count, keep, send, half, sums, ident):
    rows, before = keep.shape[1], half.shape[0]
    vmem = pl.BlockSpec(memory_space=VMEM)
    shape = jax.ShapeDtypeStruct
    return pl.pallas_call(
        functools.partial(tail_kernel, count, len(sums)),
        name="tail",
        in_specs=[pl.BlockSpec(memory_space=ANY)] * 3 + [vmem] * len(sums),
        out_specs=[vmem] * 3,
        out_shape=[shape((rows, LANES), BF), shape((before, LANES), BF), shape((8, LANES), F32)],
        scratch_shapes=near_scratch(rows, (1, 1)) + wide_scratch(before) + wide_scratch(rows)
        + [VMEM((rows, LANES), BF), VMEM((8, LANES), F32), VMEM((4, 8, LANES), F32), pltpu.SemaphoreType.DMA((2,)), pltpu.SemaphoreType.DMA((2,))],
        compiler_params=params(collective_id=ident, has_side_effects=True),
    )(keep, send, half, *sums)


def forward_kernel(runs, first, last, meanwhile, later, *refs):
    refs = list(refs)
    x_ref = refs.pop(0)
    y_in = None if first else refs.pop(0)
    slots = [refs.pop(0) for _ in range(4)]
    gate_ref, up_ref = refs.pop(0), refs.pop(0)
    outs = [refs.pop(0) for _ in range(2 if last else 1)]
    wgu, wd, prod_ref, sems = refs
    width = 4 * units(runs)

    @pl.when(pl.program_id(0) == 0)
    def _():
        fetch(slots, wgu, wd, sems, runs, meanwhile)

    later()
    wide = x_ref[...].astype(F32)
    a = (wide * scale_of(wide)).astype(BF)
    for c, n in pieces(width):
        g = dot(a, wgu[:, pl.ds(c, n)])
        u = dot(a, wgu[:, pl.ds(width + c, n)])
        gate_ref[:, pl.ds(c, n)] = g
        up_ref[:, pl.ds(c, n)] = u
        prod_ref[:, pl.ds(c, n)] = (g * sigmoid(g) * u).astype(BF)
    y = dot(prod_ref[...], wd[...])
    if not first:
        y = y + y_in[...]
    if last:
        h = (wide + y.astype(BF).astype(F32)).astype(BF)
        outs[0][...] = h
        wide = h.astype(F32)
        outs[1][...] = (wide * scale_of(wide)).astype(BF)
    else:
        outs[0][...] = y


def swiglu_back(g, u, dp):
    dp = dp.astype(BF).astype(F32)
    sig = sigmoid(g)
    act = g * sig
    return (act * u).astype(BF), (dp * u * (sig + act * (1.0 - sig))).astype(BF), (dp * act).astype(BF)


def last_kernel(runs, first, last, meanwhile, later, *refs):
    refs = list(refs)
    a_ref, dy_ref = refs.pop(0), refs.pop(0)
    da_in = None if first else refs.pop(0)
    h_ref = refs.pop(0) if last else None
    slots = [refs.pop(0) for _ in range(4)]
    out_ref, keep, send = refs.pop(0), refs.pop(0), refs.pop(0)
    wgu, wd, acc_gu, acc_d, turned, at_ref, dyt_ref, sems, dcat = refs
    width = 4 * units(runs)

    @pl.when(pl.program_id(0) == 0)
    def _():
        def clear():
            meanwhile()
            acc_gu[...] = jnp.zeros_like(acc_gu)
            acc_d[...] = jnp.zeros_like(acc_d)

        fetch(slots, wgu, wd, sems, runs, clear)

    later()
    a, dy = a_ref[...], dy_ref[...]
    at_ref[...] = a.T
    dyt_ref[...] = dy.T
    for c, n in pieces(width):
        g = dot(a, wgu[:, pl.ds(c, n)])
        u = dot(a, wgu[:, pl.ds(width + c, n)])
        dp = dot_nt(dy, wd[pl.ds(c, n), :])
        prod, dg, du = swiglu_back(g, u, dp)
        dcat[:, pl.ds(c, n)], dcat[:, pl.ds(width + c, n)] = dg, du
        acc_d[:, pl.ds(c, n)] += dot(dyt_ref[...], prod)
        acc_gu[:, pl.ds(c, n)] += dot(at_ref[...], dg)
        acc_gu[:, pl.ds(width + c, n)] += dot(at_ref[...], du)
    da = dot_nt(dcat[...], wgu[...])
    if not first:
        da = da + da_in[...]
    if last:
        da = da.astype(BF).astype(F32)
        wide = h_ref[...].astype(F32)
        scale = scale_of(wide)
        by_scale = jnp.mean(da * wide, -1, keepdims=True)
        by_h = (da * scale - wide * (scale * scale * scale * by_scale)).astype(BF)
        out_ref[...] = (dy.astype(F32) + by_h.astype(F32)).astype(BF)
    else:
        out_ref[...] = da

    @pl.when(pl.program_id(0) == pl.num_programs(0) - 1)
    def _():
        deliver(acc_gu, acc_d, turned, keep, send, runs)


def first_back_kernel(runs, meanwhile, later, *refs):
    x_ref, dh_ref, gate_ref, up_ref, *refs = refs
    slots, (keep, send, wd, acc_gu, acc_d, turned, at_ref, dht_ref, sems) = refs[:4], refs[4:]
    width = 4 * units(runs)

    @pl.when(pl.program_id(0) == 0)
    def _():
        def clear():
            meanwhile()
            acc_gu[...] = jnp.zeros_like(acc_gu)
            acc_d[...] = jnp.zeros_like(acc_d)

        fetch(slots, None, wd, sems, runs, clear)

    later()
    wide = x_ref[...].astype(F32)
    a = (wide * scale_of(wide)).astype(BF)
    dh = dh_ref[...]
    at_ref[...] = a.T
    dht_ref[...] = dh.T
    for c, n in pieces(width):
        dp = dot_nt(dh, wd[pl.ds(c, n), :])
        g, u = gate_ref[:, pl.ds(c, n)], up_ref[:, pl.ds(c, n)]
        prod, dg, du = swiglu_back(g, u, dp)
        acc_d[:, pl.ds(c, n)] += dot(dht_ref[...], prod)
        acc_gu[:, pl.ds(c, n)] += dot(at_ref[...], dg)
        acc_gu[:, pl.ds(width + c, n)] += dot(at_ref[...], du)

    @pl.when(pl.program_id(0) == pl.num_programs(0) - 1)
    def _():
        deliver(acc_gu, acc_d, turned, keep, send, runs)


def call(kernel, name, tokens, blocked, slots, outs, whole, scratch, flops, aliases=None, carried=None, half=None, wanted=None, ident=None):
    tb = TOKENS_PER_STEP
    by_token = lambda width: pl.BlockSpec((tb, width), lambda i: (i, 0))
    shape = jax.ShapeDtypeStruct
    extra, added, more, flows = [], [], [], []
    if carried:
        rows = carried[0].shape[1]
        flows.append((functools.partial(Near, (1,)), len(extra), len(added), len(more), 2, 1, 6))
        extra, more = extra + list(carried), more + near_scratch(rows, (1,))
        added = added + [shape((rows, LANES), BF)]
    if half is not None:
        flows.append((Wide, len(extra), len(added), len(more), 1, 2, 5))
        extra, more = extra + [half], more + wide_scratch(half.shape[0])
        added = added + [shape(half.shape, BF), shape((8, LANES), F32)]
    n_in, n_out = len(blocked) + len(slots), len(outs) + len(whole)
    blocks = [] if wanted is None else [wanted]
    fetched = [shape(wanted.shape, BF)] * 3 if blocks else []
    sems = fetch_scratch() if blocks else []

    def body(*refs):
        refs = list(refs)
        ins, refs = refs[:n_in], refs[n_in:]
        before, refs = refs[: len(extra)], refs[len(extra) :]
        block, refs = refs[: len(blocks)], refs[len(blocks) :]
        out, refs = refs[:n_out], refs[n_out:]
        flown, refs = refs[: len(added)], refs[len(added) :]
        there, refs = refs[: len(fetched)], refs[len(fetched) :]
        own, refs = refs[: len(scratch)], refs[len(scratch) :]
        after, sems = refs[: len(more)], refs[len(more) :]
        step = pl.program_id(0)
        going = [make(*before[i : i + a], *flown[j : j + b], *after[k : k + c]) for make, i, j, k, a, b, c in flows]
        fetching = Fetch(*block, *there, *sems) if blocks else None

        def meanwhile():
            if going or blocks:
                greet((going or [fetching])[0].targets())
            for flow in going:
                flow.enter()
            if blocks:
                fetching.start()

        def later():
            for flow in going:
                flow.at_start(step)

        kernel(meanwhile, later, *ins, *out, *own)
        for flow in reversed(going):
            flow.at_end(step)
        if blocks:
            pl.when(step == pl.num_programs(0) - 2)(fetching.forward)
            pl.when(step == pl.num_programs(0) - 1)(fetching.finish)

    nbytes = sum(b.size * b.dtype.itemsize for b in (*blocked, *slots, *outs, *whole))
    return pl.pallas_call(
        body,
        name=name,
        grid=(tokens // tb,),
        in_specs=[by_token(b.shape[1]) for b in blocked] + [pl.BlockSpec(memory_space=ANY)] * (len(slots) + len(extra) + len(blocks)),
        out_specs=[by_token(o.shape[1]) for o in outs]
        + [pl.BlockSpec(o.shape, lambda i, k=len(o.shape): (0,) * k) for o in (*whole, *added)]
        + [pl.BlockSpec(memory_space=pltpu.HBM)] * len(fetched),
        scratch_shapes=list(scratch) + more + sems,
        out_shape=[*outs, *whole, *added, *fetched],
        input_output_aliases=aliases or {},
        compiler_params=params(collective_id=ident, has_side_effects=True) if flows or blocks else params(),
        cost_estimate=pl.CostEstimate(flops=flops, bytes_accessed=nbytes, transcendentals=0),
    )(*blocked, *slots, *extra, *blocks)


def grads(width):
    return [jax.ShapeDtypeStruct((2, 15 * width // 4, LANES), BF)] * 2


def back_scratch(d, width, gu):
    tb = TOKENS_PER_STEP
    return ([VMEM((d, 2 * width), BF)] if gu else []) + [
        VMEM((width, d), BF), VMEM((d, 2 * width), F32), VMEM((d, width), F32), VMEM((width, d), BF),
        VMEM((d, tb), BF), VMEM((d, tb), BF), pltpu.SemaphoreType.DMA((2,)),
    ]


def forward_call(runs, first, last, name, x, y, slots, wanted=None, ident=None):
    tokens, d = x.shape
    width, shape = 4 * units(runs), jax.ShapeDtypeStruct
    end = [shape((tokens, d), BF)] * 2 if last else [shape((tokens, d), F32)]
    return call(
        functools.partial(forward_kernel, runs, first, last), name, tokens, [x] if first else [x, y], slots,
        [shape((tokens, width), F32)] * 2 + end, [],
        [VMEM((d, 2 * width), BF), VMEM((width, d), BF), VMEM((TOKENS_PER_STEP, width), BF), pltpu.SemaphoreType.DMA((2,))],
        6 * tokens * d * width, aliases={} if first or last else {1: 2}, wanted=wanted, ident=ident,
    )


def last_call(runs, first, last, name, a, dy, da, h, slots, carried=None, half=None, wanted=None, ident=None):
    tokens, d = a.shape
    width = 4 * units(runs)
    return call(
        functools.partial(last_kernel, runs, first, last), name, tokens,
        [a, dy] + ([] if first else [da]) + ([h] if last else []), slots,
        [jax.ShapeDtypeStruct((tokens, d), BF if last else F32)], grads(width),
        back_scratch(d, width, True) + [VMEM((TOKENS_PER_STEP, 2 * width), BF)],
        16 * tokens * d * width, aliases={} if first or last else {2: 0}, carried=carried, half=half, wanted=wanted, ident=ident,
    )


def back_call(runs, name, x, dh, gate, up, slots, carried=None, half=None, ident=None):
    tokens, d = x.shape
    width = 4 * units(runs)
    return call(
        functools.partial(first_back_kernel, runs), name, tokens, [x, dh, gate, up], slots, [], grads(width),
        back_scratch(d, width, False), 8 * tokens * d * width, carried=carried, half=half, ident=ident,
    )


def update_kernel(factor_ref, *refs):
    n = 2 * len(CHUNKS)
    blocks, packs, ins, outs, g_ref = refs[:n], refs[n : 2 * n], refs[2 * n : 2 * n + 9], refs[2 * n + 9 : 2 * n + 18], refs[2 * n + 18]
    w_down, m_down, v_down = ins[6:]
    for l in range(2):

        @pl.when(pl.program_id(0) == l)
        def _(l=l):
            for runs, block, pack in zip(CHUNKS, blocks[l * n // 2 :], packs[l * n // 2 :]):
                for i in range(2):
                    tile = i * units(runs) // 32
                    for first, size in runs:
                        if size >= LANES:
                            for s in range(4):
                                for t in range(size // LANES):
                                    g_ref[i, :, pl.ds(s * 800 + first + t * LANES, LANES)] = block[tile].astype(F32)
                                    tile += 1
                        else:
                            four = block[tile].astype(F32)
                            for s in range(4):
                                g_ref[i, :, pl.ds(s * 800 + first, size)] = four[:, s * size : (s + 1) * size]
                first, size = runs[0][0], units(runs)
                for t in range(5):

                    @pl.when(pl.program_id(1) == t)
                    def _(t=t, first=first, size=size, pack=pack):
                        at = (0, pl.ds(first, size), pl.ds(t * LANES, LANES))
                        g = pack[pl.ds((10 + t) * size, size), :].astype(F32) * factor_ref[0:1, :]
                        for o, value in zip(outs[6:], adamw(w_down[at].astype(F32), m_down[at], v_down[at], g)):
                            o[at] = value

    for i in range(2):
        w, m, v = (r[0] for r in ins[3 * i : 3 * i + 3])
        g = g_ref[i] * factor_ref[0:1, 0:1]
        for o, value in zip(outs[3 * i : 3 * i + 3], adamw(w.astype(F32), m, v, g)):
            o[0] = value


def adamw(w, m, v, g):
    m = 0.9 * m + 0.1 * g
    v = 0.95 * v + 0.05 * g * g
    step = m * lax.rsqrt(v + 1e-8) + 0.1 * w
    return (w - 0.02 * step).astype(BF), m, v


def solution(mesh):
    def step(x, dy, w_gate, w_up, w_down, *moments):
        x, dy = x[0], dy[0]
        tokens, d = x.shape
        shape = jax.ShapeDtypeStruct
        n = len(CHUNKS)

        order = list(reversed(range(n)))
        wanted = [(0, j) for j in order] + [(1, j) for j in range(n)]
        got = open_call(wanted, w_gate, w_up, w_down, 0)
        own, there = got[: 2 * n], got[2 * n :]
        slots = {wanted[0]: (own[0], *there)}
        kept, y = {}, None
        for k, j in enumerate(order):
            gate, up, *got = forward_call(CHUNKS[j], k == 0, k == n - 1, f"forward0_{j}", x, y, slots[0, j], own[k + 1], 1 + k)
            kept[j] = gate, up
            y, there = got[0], got[-3:]
            slots[wanted[k + 1]] = (own[k + 1], *there)
        h, a = got[:2]

        every, squares, pair, half, da = [], [], None, None, None
        for l, j in [(1, j) for j in range(n)] + [(0, j) for j in range(n)]:
            more = None
            if l:
                more = None if j == n - 1 else own[n + j + 1]
                got = last_call(CHUNKS[j], j == 0, j == n - 1, f"layer1_{j}", a, dy, da, h, slots[1, j], pair, half, more, 1 + n + j)
                da, *got = got
            else:
                got = back_call(CHUNKS[j], f"back0_{j}", x, da, *kept[j], slots[0, j], pair, half, 1 + 2 * n + j)
            new, got = got[:2], list(got[2:])
            new_half = got.pop(0) if pair else None
            if half is not None:
                every, squares = every + [got.pop(0)], squares + [got.pop(0)]
            if more is not None:
                slots[1, j + 1] = (more, *got)
            pair, half = new, new_half
        count = 4 * (sum(g.size for g in every) + half.size + pair[0].size // 2)
        g, before, factor = tail_call(count, *pair, half, squares, 1 + 3 * n)
        every = every[n:] + [before, g] + every[:n]

        m, v = moments[:3], moments[3:]
        smem = pl.BlockSpec(memory_space=VMEM)
        rows, block = w_gate.shape[1], 32
        packs = [g.reshape(-1, rows, LANES) for g in every]

        def pack_spec(g, l):
            def index(i, k):
                return (0, jnp.where(i == l, k, 0 if l else rows // block - 1), 0)
            return pl.BlockSpec((2 * g.shape[0] // 3, block, LANES), index)

        gu_spec = pl.BlockSpec((1, block, w_gate.shape[2]), lambda i, k: (i, k, 0))
        gu_shapes = [shape(w_gate.shape, t) for t in (BF, F32, F32)] * 2
        d_spec = pl.BlockSpec((1, *w_down.shape[1:]), lambda i, k: (i, 0, 0))
        out = pl.pallas_call(
            update_kernel,
            name="update",
            grid=(2, rows // block),
            in_specs=[smem]
            + [pack_spec(g, i // n) for i, g in enumerate(packs)]
            + [pl.BlockSpec(g.shape, lambda i, k: (0, 0)) for g in every]
            + [gu_spec] * 6 + [d_spec] * 3,
            out_specs=[gu_spec] * 6 + [d_spec] * 3,
            out_shape=gu_shapes + [shape(w_down.shape, t) for t in (BF, F32, F32)],
            scratch_shapes=[VMEM((2, block, w_gate.shape[2]), F32)],
            compiler_params=params(),
        )(factor, *packs, *every, w_gate, m[0], v[0], w_up, m[1], v[1], w_down, m[2], v[2])
        return tuple(out[3 * i + k] for k in range(3) for i in range(3))

    states, cut = P(("rep", "r", "s"), None, None), P(None, "s", None)
    return jax.shard_map(
        step,
        mesh=mesh,
        in_specs=(states, states) + (cut,) * 9,
        out_specs=(P("rep", "s", None),) * 9,
        check_vma=False,
    )
```
